256 devices in a mesh: dp: 8 (over z), seq: 8 (over x, core), mp: 4 (over y).
Axes of the slice: x: 4, y: 4, z: 8, core: 2. Of those that a mesh axis runs over, the one named last changes fastest.
Arguments:
- frames_in: bfloat16 [32, 2048, 512], P('dp', 'seq'), may hold values from -6 to 6
- lengths: int32 [32], P('dp'), may hold values from 32 to 2048, as said below
- attn_gain: float32 [2, 512], replicated, may hold values from 0.25 to 1.75
- ffn_gain: float32 [2, 512], replicated, may hold values from 0.25 to 1.75
- qkv_weight: bfloat16 [2, 3, 512, 512], P(None, None, ('dp', 'seq'), 'mp'), may hold values from -1.5 to 1.5
- out_weight: bfloat16 [2, 512, 512], P(None, ('dp', 'seq'), 'mp'), may hold values from -0.25 to 0.25
- up_weight: bfloat16 [2, 512, 2048], P(None, ('dp', 'seq'), 'mp'), may hold values from -0.25 to 0.25
- down_weight: bfloat16 [2, 512, 2048], P(None, ('dp', 'seq'), 'mp'), may hold values from -0.125 to 0.125
Outputs:
- encoded: bfloat16 [32, 2048, 512], P('dp', 'seq')
The draws below stay inside these ranges and needn't reach their ends.
Inputs may be any that keep to these rules, and one draw needn't show every extreme that they name: `lengths`: each utterance's number of valid frames is a multiple of 32; frames from there on are padding; in every draw some utterance has all 2048 frames valid.
All inputs are finite; a program needn't handle non-finite values.
Results may differ from the reference program's by a relative error of at most 0.02.
Values may be sent and summed in bfloat16 or wider, within the bound.
No kernel may reach another device: no remote copies, remote signals or barrier semaphores. Data moves between devices by JAX's collectives and lax.ppermute only.
A program may use at most 64 MiB of HBM per device.

```python
import jax
import jax.numpy as jnp
from jax import lax

D = 512
HEADS = 8
FF = 2048
HEAD_DIM = 64
STRETCH = 32
LEFT = 64
MEMORY = 4
LAYERS = 2
BATCH = 32
STRETCHES = 64
FRAMES = 2048
N_MP = 4


def shared_mean(key):
    mean_key = jax.random.fold_in(key, 31)
    mean_vector = jax.random.normal(mean_key, (D,), jnp.float32)
    return mean_vector - jnp.mean(mean_vector)


def draw_frames_in(key, part):
    mean_vector = shared_mean(key)
    span_key = jax.random.fold_in(key, 32)
    noise_key = jax.random.fold_in(key, 33)
    span_part = jax.random.normal(span_key, (BATCH, STRETCHES, D), jnp.float32)
    noise = jax.random.normal(noise_key, (BATCH, FRAMES, D), jnp.float32)
    values = 0.6 * mean_vector[None, None, :] + 0.4 * jnp.repeat(span_part, STRETCH, axis=1) + noise
    return jnp.clip(values, -6.0, 6.0).astype(jnp.bfloat16)


def draw_lengths(key, part):
    count_key = jax.random.fold_in(key, 11)
    full_key = jax.random.fold_in(key, 12)
    stretch_counts = jax.random.randint(count_key, (BATCH,), 1, STRETCHES + 1)
    full_slot = jax.random.randint(full_key, (), 0, BATCH)
    stretch_counts = jnp.where(jnp.arange(BATCH) == full_slot, STRETCHES, stretch_counts)
    return (stretch_counts * STRETCH).astype(jnp.int32)


def draw_qkv_weight(key, part):
    mean_vector = shared_mean(key)
    direction = mean_vector / jnp.sqrt(jnp.sum(mean_vector * mean_vector))
    normal_key = jax.random.fold_in(key, 21)
    head_key = jax.random.fold_in(key, 22)
    shared_key = jax.random.fold_in(key, 23)
    sample_values = jax.random.normal(normal_key, (LAYERS, 3, D, D), jnp.float32) * D ** (-0.5)
    head_scale = jax.random.uniform(head_key, (LAYERS, HEADS), jnp.float32, 1.7, 2.3)
    column_scale = jnp.repeat(head_scale, D // HEADS, axis=1)
    shared_row = jax.random.normal(shared_key, (LAYERS, D), jnp.float32) * column_scale * D ** (-0.5)
    aligned = direction[None, :, None] * shared_row[:, None, :]
    query_part = sample_values[:, 0] + aligned
    key_part = sample_values[:, 1] + aligned
    sample_values = jnp.stack([query_part, key_part, sample_values[:, 2]], axis=1)
    return jnp.clip(sample_values, -1.5, 1.5).astype(jnp.bfloat16)


def block_scale(stream_key, shape, shards, smallest, top_value):
    def one(axis_at, shards_of):
        steps = jax.random.uniform(jax.random.fold_in(jax.random.fold_in(stream_key, 6), axis_at), (shards_of,), jnp.float32, smallest / len(shards), top_value / len(shards))
        return jnp.repeat(jnp.exp(steps), shape[axis_at] // shards_of).reshape((-1,) + (1,) * (len(shape) - axis_at - 1))

    loudness = one(*shards[0])
    for cut in shards[1:]:
        loudness = loudness * one(*cut)
    return loudness


def bell_draw(own_key, extent, width, bound, pieces=(), kind=jnp.bfloat16):
    drawn = width * jax.random.normal(own_key, extent, jnp.float32)
    if pieces:
        drawn = drawn * block_scale(own_key, extent, pieces, -0.22, 0.18)
    return jnp.clip(drawn, -bound, bound).astype(kind)


def setup_inputs(seed: int = 0) -> dict:
    arg_keys = jax.random.split(jax.random.key(seed), 9)
    frames_in = draw_frames_in(jax.random.fold_in(arg_keys[8], 71), 0)
    lengths = draw_lengths(jax.random.fold_in(arg_keys[8], 71), 0)
    attn_gain = jnp.clip(1.0 + 0.15 * jax.random.normal(arg_keys[2], (LAYERS, D), jnp.float32), 0.25, 1.75)
    ffn_gain = jnp.clip(1.0 + 0.15 * jax.random.normal(arg_keys[3], (LAYERS, D), jnp.float32), 0.25, 1.75)
    qkv_weight = draw_qkv_weight(jax.random.fold_in(arg_keys[8], 71), 0)
    out_weight = bell_draw(arg_keys[5], (LAYERS, D, D), D ** -0.5, 0.25, ((1, 64), (2, 4)))
    up_weight = bell_draw(arg_keys[6], (LAYERS, D, FF), D ** -0.5, 0.25, ((1, 64), (2, 4)))
    down_weight = bell_draw(arg_keys[7], (LAYERS, D, FF), FF ** -0.5, 0.125, ((1, 64), (2, 4)))
    return {"frames_in": frames_in, "lengths": lengths, "attn_gain": attn_gain, "ffn_gain": ffn_gain, "qkv_weight": qkv_weight, "out_weight": out_weight, "up_weight": up_weight, "down_weight": down_weight}


epsilon = 1e-05
masked_score = -1e+30

def layer_norm(values, gain_row):
    average = lax.optimization_barrier(jnp.mean(values, axis=-1, keepdims=True))
    centred = values - average
    spread = lax.optimization_barrier(jnp.mean(centred * centred, axis=-1, keepdims=True))
    return (centred * lax.rsqrt(spread + epsilon) * gain_row).astype(jnp.bfloat16)

def stretch_mean(values, stretch_rows):
    row_count, model_width = values.shape
    shaped = values.reshape(stretch_rows, row_count // stretch_rows, model_width)
    return lax.optimization_barrier(jnp.mean(shaped, axis=1, dtype=jnp.float32))

def back_product(inputs, weight):
    return lax.dot_general(inputs, weight, (((1,), (1,)), ((), ())), preferred_element_type=jnp.float32)

def grouped_back(inputs, weight):
    group_width = inputs.shape[1] // N_MP
    running = jnp.zeros((inputs.shape[0], weight.shape[0]), jnp.float32)
    for group_index in range(N_MP):
        lower = group_index * group_width
        term_part = back_product(inputs[:, lower:lower + group_width], weight[:, lower:lower + group_width])
        rounded = lax.optimization_barrier(term_part.astype(jnp.bfloat16))
        running = running + rounded.astype(jnp.float32)
    return running

def attend(query_frames, query_summary, key_ext, value_ext, keymem_ext, valmem_ext, first_stretch):
    utterances, ext_frames, head_cols = key_ext.shape
    groups = query_summary.shape[1]
    head_count = head_cols // HEAD_DIM
    blocks = LEFT // STRETCH + 1
    slots = MEMORY + blocks * STRETCH

    def gather_slots(frame_ext, memory_ext):
        frame_blocks = frame_ext.reshape(utterances, ext_frames // STRETCH, STRETCH, head_cols)
        frame_part = jnp.stack([frame_blocks[:, offset:offset + groups] for offset in range(blocks)], axis=2)
        frame_part = frame_part.reshape(utterances, groups, blocks * STRETCH, head_count, HEAD_DIM)
        memory_part = jnp.stack([memory_ext[:, offset:offset + groups] for offset in range(MEMORY)], axis=2)
        memory_part = memory_part.reshape(utterances, groups, MEMORY, head_count, HEAD_DIM)
        return jnp.concatenate([memory_part, frame_part], axis=2)
    all_keys = gather_slots(key_ext, keymem_ext).astype(jnp.float32)
    all_values = gather_slots(value_ext, valmem_ext).astype(jnp.float32)
    queries = jnp.concatenate([query_frames.reshape(utterances, groups, STRETCH, head_cols), query_summary[:, :, None, :]], axis=2)
    queries = queries.reshape(utterances, groups, STRETCH + 1, head_count, HEAD_DIM).astype(jnp.float32)
    scores = jnp.einsum('bcqhe,bckhe->bchqk', queries, all_keys) * HEAD_DIM ** (-0.5)
    stretch_index = first_stretch + jnp.arange(groups, dtype=jnp.int32)
    slot_index = jnp.arange(slots, dtype=jnp.int32)
    memory_source = stretch_index[:, None] - MEMORY + slot_index[None, :]
    frame_source = stretch_index[:, None] - (blocks - 1) + (slot_index[None, :] - MEMORY) // STRETCH
    source = jnp.where(slot_index[None, :] < MEMORY, memory_source, frame_source)
    allowed = source >= 0
    scores = jnp.where(allowed[None, :, None, None, :], scores, masked_score)
    highest = lax.optimization_barrier(jnp.max(scores, axis=-1, keepdims=True))
    exponent = jnp.exp(scores - highest)
    probs = (exponent / lax.optimization_barrier(jnp.sum(exponent, axis=-1, keepdims=True))).astype(jnp.bfloat16)
    mixed = jnp.einsum('bchqk,bckhe->bcqhe', probs.astype(jnp.float32), all_values).astype(jnp.bfloat16)
    mixed = mixed.reshape(utterances, groups, STRETCH + 1, head_cols)
    frame_out = mixed[:, :, :STRETCH].reshape(utterances * groups * STRETCH, head_cols)
    summary_out = mixed[:, :, STRETCH].reshape(utterances * groups, head_cols)
    return (frame_out, summary_out)

def reference(frames_in, lengths, attn_gain, ffn_gain, qkv_weight, out_weight, up_weight, down_weight):
    batch_count, frame_count, model_width = frames_in.shape
    stretch_count = frame_count // STRETCH
    row_count = batch_count * frame_count
    stretch_rows = batch_count * stretch_count
    flat_in = frames_in.reshape(row_count, model_width)
    residual = flat_in.astype(jnp.float32)
    memory = stretch_mean(flat_in, stretch_rows)
    for layer_index in range(LAYERS):
        normed = layer_norm(residual, attn_gain[layer_index])
        mem_normed = layer_norm(memory, attn_gain[layer_index])
        summary = stretch_mean(normed, stretch_rows).astype(jnp.bfloat16)
        weights = qkv_weight[layer_index]
        queries = jnp.dot(normed, weights[0], preferred_element_type=jnp.float32).astype(jnp.bfloat16)
        query_sum = jnp.dot(summary, weights[0], preferred_element_type=jnp.float32).astype(jnp.bfloat16)
        key_frames = jnp.dot(normed, weights[1], preferred_element_type=jnp.float32).astype(jnp.bfloat16)
        value_frames = jnp.dot(normed, weights[2], preferred_element_type=jnp.float32).astype(jnp.bfloat16)
        key_memory = jnp.dot(mem_normed, weights[1], preferred_element_type=jnp.float32).astype(jnp.bfloat16)
        value_memory = jnp.dot(mem_normed, weights[2], preferred_element_type=jnp.float32).astype(jnp.bfloat16)
        left_zeros = jnp.zeros((batch_count, LEFT, model_width), jnp.bfloat16)
        memory_zeros = jnp.zeros((batch_count, MEMORY, model_width), jnp.bfloat16)
        key_ext = jnp.concatenate([left_zeros, key_frames.reshape(batch_count, frame_count, model_width)], axis=1)
        value_ext = jnp.concatenate([left_zeros, value_frames.reshape(batch_count, frame_count, model_width)], axis=1)
        keymem_ext = jnp.concatenate([memory_zeros, key_memory.reshape(batch_count, stretch_count, model_width)], axis=1)
        valmem_ext = jnp.concatenate([memory_zeros, value_memory.reshape(batch_count, stretch_count, model_width)], axis=1)
        frame_out, summary_out = attend(queries.reshape(batch_count, frame_count, model_width), query_sum.reshape(batch_count, stretch_count, model_width), key_ext, value_ext, keymem_ext, valmem_ext, 0)
        residual = residual + grouped_back(frame_out, out_weight[layer_index])
        memory = grouped_back(summary_out, out_weight[layer_index])
        ffn_in = layer_norm(residual, ffn_gain[layer_index])
        hidden = jax.nn.gelu(jnp.dot(ffn_in, up_weight[layer_index], preferred_element_type=jnp.float32), approximate=False).astype(jnp.bfloat16)
        residual = residual + grouped_back(hidden, down_weight[layer_index])
    position = jnp.arange(frame_count, dtype=jnp.int32)
    keep = position[None, :] < lengths[:, None]
    encoded = jnp.where(keep[:, :, None], residual.reshape(batch_count, frame_count, model_width), 0.0).astype(jnp.bfloat16)
    return encoded
```

```python
import jax
import jax.numpy as jnp
from jax import lax
from jax.experimental import pallas as pl
from jax.experimental.pallas import tpu as pltpu
from jax.sharding import PartitionSpec as P

HEAD_DIM = 64
STRETCH = 32
LEFT = 64
MEMORY = 4
EPS = 1e-05
MASKED = -1e30
PIECE_FROM = (0, -1, 1, 2)
F32 = jnp.float32
BF16 = jnp.bfloat16

ROWS = 256
GROUPS = ROWS // STRETCH
D = 512
FF = 2048
PRIOR = LEFT + 16
KEYS = 384
QUERIES = ROWS + 16
VMEM = pl.BlockSpec(memory_space=pltpu.VMEM)
SMEM = pl.BlockSpec(memory_space=pltpu.SMEM)
HBM = pl.BlockSpec(memory_space=pltpu.HBM)


def norm(values, gain):
    average = jnp.mean(values, axis=-1, keepdims=True)
    centred = values - average
    spread = jnp.mean(centred * centred, axis=-1, keepdims=True)
    return (centred * lax.rsqrt(spread + EPS) * gain).astype(BF16)


def stretch_mean(values):
    return jnp.mean(values.reshape(GROUPS, STRETCH, D), axis=1)


def enter_layer(x, memory, gain, xn_ref, ms_ref, tail_ref):
    xn = norm(x, gain)
    mn = norm(memory, gain).astype(F32)
    summary = stretch_mean(xn.astype(F32))
    zeros8 = jnp.zeros((8, D), F32)
    xn_ref[...] = xn
    ms_ref[0:16, :] = jnp.concatenate([mn, zeros8], axis=0).astype(BF16)
    ms_ref[16:32, :] = jnp.concatenate([summary, zeros8], axis=0).astype(BF16)
    tail_ref[0:LEFT, :] = xn[ROWS - LEFT :]
    last = jnp.concatenate([mn[GROUPS - MEMORY :], jnp.zeros((16 - MEMORY, D), F32)], axis=0)
    tail_ref[LEFT:PRIOR, :] = last.astype(BF16)


def first_kernel(where_ref, frames_ref, gain_ref, x_ref, xn_ref, ms_ref, tail_ref, buf, sem):
    copy = pltpu.make_async_copy(frames_ref.at[where_ref[0]], buf, sem)
    copy.start()
    copy.wait()
    x = buf[...].astype(F32)
    x_ref[...] = x
    enter_layer(x, stretch_mean(x), gain_ref[0:1, :], xn_ref, ms_ref, tail_ref)


def first_step(where, frames_in, attn_gain):
    return pl.pallas_call(
        first_kernel,
        out_shape=(
            jax.ShapeDtypeStruct((ROWS, D), F32),
            jax.ShapeDtypeStruct((ROWS, D), BF16),
            jax.ShapeDtypeStruct((32, D), BF16),
            jax.ShapeDtypeStruct((PRIOR, D), BF16),
        ),
        in_specs=[SMEM, HBM, VMEM],
        out_specs=(VMEM, VMEM, VMEM, VMEM),
        scratch_shapes=[pltpu.VMEM((ROWS, D), BF16), pltpu.SemaphoreType.DMA],
        name="first_step",
    )(where, frames_in, attn_gain)


def back_product(inputs, weight):
    return lax.dot_general(inputs, weight, (((1,), (1,)), ((), ())), preferred_element_type=F32)


def gelu(values):
    return 0.5 * values * (1.0 + lax.erf(values * (2.0**-0.5)))


def layer_kernel(last, layer, where_ref, x_ref, xn_ref, ms_ref, prior_ref, fgain_ref, again_ref, *rest):
    pieces, rest = rest[:16], rest[16:]
    if last:
        out_ref, *scratch = rest
    else:
        x_out, xn_out, ms_out, tail_out, *scratch = rest
    w, kin, qin, ks, vs, qs, os_, bias, sems = scratch
    core, x_at, y_at = where_ref[3], where_ref[4], where_ref[5]

    def fetch(arrays):
        for sem, group in ((0, slice(0, 4)), (1, slice(4, 12))):
            for k, by in enumerate(PIECE_FROM):
                for half in range(2):
                    src = arrays[2 * k + half].reshape(4, 4, 12, 16, 128)
                    z_rows = slice(4 * half, 4 * half + 4)
                    if layer == 0:
                        cols = pl.ds(pl.multiple_of(((y_at + by) & 3) * 128, 128), 128)
                        dst = w.at[z_rows, :, group, :, cols]
                        pltpu.make_async_copy(src.at[:, :, group], dst, sems.at[sem]).start()
                    else:
                        for y in range(4):
                            dst = w.at[z_rows, (x_at + by) & 3, group, :, 128 * y : 128 * y + 128]
                            pltpu.make_async_copy(src.at[:, y, group], dst, sems.at[sem]).start()

    @pl.when(core == layer)
    def _():
        fetch(pieces[:8])

    @pl.when(core != layer)
    def _():
        fetch(pieces[8:])

    def arrived(sem, group):
        pltpu.make_async_copy(w.at[:, :, group], w.at[:, :, group], sems.at[sem]).wait()

    def matrix(j):
        return w[:, :, j].reshape(D, D)

    first_stretch = where_ref[1]
    kin[0:LEFT, :] = prior_ref[0:LEFT, :]
    kin[LEFT : LEFT + ROWS, :] = xn_ref[...]
    kin[320:336, :] = prior_ref[LEFT:PRIOR, :]
    kin[336:352, :] = ms_ref[0:16, :]
    kin[352:384, :] = jnp.zeros((32, D), BF16)
    qin[0:ROWS, :] = xn_ref[...]
    qin[ROWS:QUERIES, :] = ms_ref[16:32, :]
    row = lax.broadcasted_iota(jnp.int32, (QUERIES, KEYS), 0)
    col = lax.broadcasted_iota(jnp.int32, (QUERIES, KEYS), 1)
    stretch = jnp.where(row < ROWS, row // STRETCH, (row - ROWS) % GROUPS)
    frame_from = col // STRETCH - LEFT // STRETCH
    memory_from = jnp.where(col < 336, col - 320 - MEMORY, col - 336)
    memory_there = col < jnp.where(col < 336, 320 + MEMORY, 336 + GROUPS)
    is_frame = col < LEFT + ROWS
    source = jnp.where(is_frame, frame_from, memory_from)
    back = stretch - source
    seen_frame = is_frame & (back >= 0) & (back <= LEFT // STRETCH)
    seen_memory = (~is_frame) & memory_there & (back >= 1) & (back <= MEMORY)
    allowed = (seen_frame | seen_memory) & (source + first_stretch >= 0)
    bias[...] = jnp.where(allowed, 0.0, MASKED)

    arrived(0, slice(0, 4))
    q = jnp.dot(qin[...], matrix(0), preferred_element_type=F32)
    qs[...] = (q * HEAD_DIM ** (-0.5)).astype(BF16)
    ks[...] = jnp.dot(kin[...], matrix(1), preferred_element_type=F32).astype(BF16)
    vs[...] = jnp.dot(kin[...], matrix(2), preferred_element_type=F32).astype(BF16)
    lane = lax.broadcasted_iota(jnp.int32, (QUERIES, 128), 1)
    for pair in range(D // 128):
        cols = slice(128 * pair, 128 * pair + 128)
        queries, keys, values = qs[:, cols], ks[:, cols], vs[:, cols]
        mixed = []
        for half in range(2):
            mine = (lane < HEAD_DIM) if half == 0 else (lane >= HEAD_DIM)
            scores = back_product(jnp.where(mine, queries, jnp.zeros_like(queries)), keys) + bias[...]
            highest = jnp.max(scores, axis=-1, keepdims=True)
            exponent = jnp.exp(scores - highest)
            total = jnp.sum(exponent, axis=-1, keepdims=True)
            product = jnp.dot(exponent.astype(BF16), values, preferred_element_type=F32)
            mixed.append(product * (1.0 / total))
        os_[:, cols] = jnp.where(lane < HEAD_DIM, mixed[0], mixed[1]).astype(BF16)
    projected = back_product(os_[...], matrix(3))
    x = x_ref[...] + projected[0:ROWS]
    hn = norm(x, fgain_ref[layer : layer + 1, :])
    arrived(1, slice(4, 12))
    for part in range(4):
        hidden = gelu(jnp.dot(hn, matrix(4 + part), preferred_element_type=F32)).astype(BF16)
        x = x + back_product(hidden, matrix(8 + part))
    if last:
        length = where_ref[2]
        position = STRETCH * first_stretch + lax.broadcasted_iota(jnp.int32, (ROWS, D), 0)
        out_ref[...] = jnp.where(position < length, x, 0.0).astype(BF16)
    else:
        x_out[...] = x
        memory = projected[ROWS : ROWS + GROUPS]
        enter_layer(x, memory, again_ref[layer + 1 : layer + 2, :], xn_out, ms_out, tail_out)


def layer_step(layer, last, where, x, xn, ms, prior, ffn_gain, attn_gain, weights):
    def kernel(*refs):
        layer_kernel(last, layer, *refs)

    if last:
        out_shape = jax.ShapeDtypeStruct((ROWS, D), BF16)
        out_specs = VMEM
    else:
        out_shape = (
            jax.ShapeDtypeStruct((ROWS, D), F32),
            jax.ShapeDtypeStruct((ROWS, D), BF16),
            jax.ShapeDtypeStruct((32, D), BF16),
            jax.ShapeDtypeStruct((PRIOR, D), BF16),
        )
        out_specs = (VMEM, VMEM, VMEM, VMEM)
    return pl.pallas_call(
        kernel,
        out_shape=out_shape,
        in_specs=[SMEM, VMEM, VMEM, VMEM, VMEM, VMEM, VMEM] + [HBM] * 16,
        out_specs=out_specs,
        scratch_shapes=[
            pltpu.VMEM((8, 4, 12, 16, D), BF16),
            pltpu.VMEM((KEYS, D), BF16),
            pltpu.VMEM((QUERIES, D), BF16),
            pltpu.VMEM((KEYS, D), BF16),
            pltpu.VMEM((KEYS, D), BF16),
            pltpu.VMEM((QUERIES, D), BF16),
            pltpu.VMEM((QUERIES, D), BF16),
            pltpu.VMEM((QUERIES, KEYS), F32),
            pltpu.SemaphoreType.DMA((2,)),
        ],
        compiler_params=pltpu.CompilerParams(vmem_limit_bytes=32 * 1024 * 1024),
        name="layer_step_%d" % layer,
    )(where, x, xn, ms, prior, ffn_gain, attn_gain, *weights)


def from_behind(array):
    devices = lax.axis_size("seq")
    return lax.ppermute(array, "seq", [(i, i + 1) for i in range(devices - 1)])


def weight_blocks(qkv_weight, out_weight, up_weight, down_weight):
    def wide(weight):
        return jnp.moveaxis(weight.reshape(2, 8, 4, 128), 2, 1)

    return jnp.concatenate([qkv_weight, out_weight[:, None], wide(up_weight), wide(down_weight)], axis=1)


def by_chip(move):
    pairs = []
    for x in range(4):
        for core in range(2):
            for y in range(4):
                to_x, to_core, to_y = move(x, core, y)
                pairs.append(((2 * x + core) * 4 + y, (2 * (to_x % 4) + to_core) * 4 + to_y % 4))
    return pairs


def to_partner(array):
    return lax.ppermute(array, ("seq", "mp"), by_chip(lambda x, core, y: (x, 1 - core, y)))


def around(array, along_x_core, by):
    def move(x, core, y):
        return (x + by, core, y) if core == along_x_core else (x, core, y + by)

    return lax.ppermute(array, ("seq", "mp"), by_chip(move))


def along_mp(array, by):
    return lax.ppermute(array, "mp", [(y, (y + by) % 4) for y in range(4)])


def all_four(low, high, send):
    from_behind_low = send(low, 1)
    from_ahead_high = send(high, -1)
    from_behind_high = send(high, 1)
    from_ahead_low = send(low, -1)
    far_low = send(from_behind_low, 1)
    far_high = send(from_ahead_high, -1)
    return [low, high, from_behind_low, from_behind_high, from_ahead_low, from_ahead_high, far_low, far_high]


def join_z_kernel(where_ref, *refs):
    pieces, (low, high) = refs[:8], refs[8:]
    for by in range(8):
        at = (where_ref[6] - by) & 7

        @pl.when(at < 4)
        def _(by=by, at=at):
            low[pl.ds(at * 12, 12)] = pieces[by][...]

        @pl.when(at >= 4)
        def _(by=by, at=at):
            high[pl.ds((at - 4) * 12, 12)] = pieces[by][...]


def join_z(where, pieces):
    half = jax.ShapeDtypeStruct((48, 16, 128), BF16)
    return pl.pallas_call(
        join_z_kernel,
        out_shape=(half, half),
        in_specs=[SMEM] + [VMEM] * 8,
        out_specs=(VMEM, VMEM),
        name="join_z",
    )(where, *pieces)


def join_ring_kernel(where_ref, *refs):
    pieces, outs = refs[:8], refs[8:]
    own = jnp.where(where_ref[3] == 0, where_ref[4], where_ref[5])
    for k, by in enumerate(PIECE_FROM):
        at = (own + by) & 3
        for half in range(2):
            for z in range(4):
                outs[half][pl.ds((4 * z + at) * 12, 12)] = pieces[2 * k + half][12 * z : 12 * z + 12]


def join_ring(where, pieces):
    half = jax.ShapeDtypeStruct((192, 16, 128), BF16)
    return pl.pallas_call(
        join_ring_kernel,
        out_shape=(half, half),
        in_specs=[SMEM] + [VMEM] * 8,
        out_specs=(VMEM, VMEM),
        name="join_ring",
    )(where, *pieces)


def join_rows_kernel(where_ref, *refs):
    pieces, out, sem = refs[:8], refs[8], refs[9]
    copies = []
    for k, by in enumerate(PIECE_FROM):
        at = (where_ref[5] + by) & 3
        for half in range(2):
            dst = out.at[at, ROWS // 2 * half : ROWS // 2 * half + ROWS // 2]
            copies.append(pltpu.make_async_copy(pieces[2 * k + half], dst, sem.at[2 * k + half]))
    for copy in copies:
        copy.start()
    for copy in copies:
        copy.wait()


def join_rows(where, pieces):
    return pl.pallas_call(
        join_rows_kernel,
        out_shape=jax.ShapeDtypeStruct((4, ROWS, D), BF16),
        in_specs=[SMEM] + [VMEM] * 8,
        out_specs=HBM,
        scratch_shapes=[pltpu.SemaphoreType.DMA((8,))],
        name="join_rows",
    )(where, *pieces)


def gather_weights(where, core, blocks):
    mine = lax.dynamic_index_in_dim(blocks, core, 0, keepdims=False)
    other = to_partner(lax.dynamic_index_in_dim(blocks, 1 - core, 0, keepdims=False))
    first = jnp.where(core == 0, mine, other)
    second = jnp.where(core == 0, other, mine)
    both = jnp.concatenate([first, second], axis=1)
    over_z = [both] + [lax.ppermute(both, "dp", [(z, (z + by) % 8) for z in range(8)]) for by in range(1, 8)]
    low, high = join_z(where, over_z)
    ring = all_four(low, high, lambda array, by: around(array, 0, by))
    low, high = join_ring(where, ring)
    pieces = all_four(low, high, lambda array, by: around(array, 1, by))
    return pieces + [to_partner(piece) for piece in pieces]


def shards(frames_in, lengths, attn_gain, ffn_gain, qkv_weight, out_weight, up_weight, down_weight):
    mp_slot = lax.axis_index("mp")
    seq_rank = lax.axis_index("seq")
    core = seq_rank % 2
    where = jnp.stack(
        [mp_slot, seq_rank * GROUPS, lengths[mp_slot], core, seq_rank // 2, mp_slot, lax.axis_index("dp")]
    ).astype(jnp.int32)
    blocks = weight_blocks(qkv_weight, out_weight, up_weight, down_weight)
    weights = gather_weights(where, core, blocks)
    x, xn, ms, tail = first_step(where, frames_in, attn_gain)
    prior = from_behind(tail)
    x, xn, ms, tail = layer_step(0, False, where, x, xn, ms, prior, ffn_gain, attn_gain, weights)
    prior = from_behind(tail)
    encoded = layer_step(1, True, where, x, xn, ms, prior, ffn_gain, attn_gain, weights)
    return join_rows(where, all_four(encoded[: ROWS // 2], encoded[ROWS // 2 :], along_mp))


def solution(mesh):
    in_specs = (
        P("dp", "seq", None),
        P("dp"),
        P(),
        P(),
        P(None, None, ("dp", "seq"), "mp"),
        P(None, ("dp", "seq"), "mp"),
        P(None, ("dp", "seq"), "mp"),
        P(None, ("dp", "seq"), "mp"),
    )
    out_specs = P("dp", "seq", None)
    return jax.shard_map(shards, mesh=mesh, in_specs=in_specs, out_specs=out_specs, check_vma=False)
```

```python
import jax
import jax.numpy as jnp
from jax import lax
from jax.experimental import pallas as pl
from jax.experimental.pallas import tpu as pltpu
from jax.sharding import PartitionSpec as P

HEAD_DIM = 64
STRETCH = 32
LEFT = 64
MEMORY = 4
EPS = 1e-05
MASKED = -1e30
PIECES = ((0, 0, 8), (-1, 0, 8), (1, 0, 8), (2, 0, 4), (2, 4, 8))
F32 = jnp.float32
BF16 = jnp.bfloat16

ROWS = 256
GROUPS = ROWS // STRETCH
D = 512
FF = 2048
PRIOR = LEFT + 16
KEYS = 384
QUERIES = ROWS + 16
VMEM = pl.BlockSpec(memory_space=pltpu.VMEM)
SMEM = pl.BlockSpec(memory_space=pltpu.SMEM)
HBM = pl.BlockSpec(memory_space=pltpu.HBM)
SMALL = pltpu.CompilerParams(vmem_limit_bytes=8 * 1024 * 1024)


def norm(values, gain):
    average = jnp.mean(values, axis=-1, keepdims=True)
    centred = values - average
    spread = jnp.mean(centred * centred, axis=-1, keepdims=True)
    return (centred * lax.rsqrt(spread + EPS) * gain).astype(BF16)


def stretch_mean(values):
    return jnp.mean(values.reshape(GROUPS, STRETCH, D), axis=1)


def enter_layer(x, memory, gain, xn_ref, ms_ref, tail_ref):
    xn = norm(x, gain)
    mn = norm(memory, gain).astype(F32)
    summary = stretch_mean(xn.astype(F32))
    zeros8 = jnp.zeros((8, D), F32)
    xn_ref[...] = xn
    ms_ref[0:16, :] = jnp.concatenate([mn, zeros8], axis=0).astype(BF16)
    ms_ref[16:32, :] = jnp.concatenate([summary, zeros8], axis=0).astype(BF16)
    tail_ref[0:LEFT, :] = xn[ROWS - LEFT :]
    last = jnp.concatenate([mn[GROUPS - MEMORY :], jnp.zeros((16 - MEMORY, D), F32)], axis=0)
    tail_ref[LEFT:PRIOR, :] = last.astype(BF16)


def place():
    seq = lax.axis_index("seq")
    return seq & 1, seq >> 1, lax.axis_index("mp"), lax.axis_index("dp"), seq


def first_kernel(frames_ref, gain_ref, x_ref, xn_ref, ms_ref, tail_ref, buf, sem):
    copy = pltpu.make_async_copy(frames_ref.at[lax.axis_index("mp")], buf, sem)
    copy.start()
    copy.wait()
    x = buf[...].astype(F32)
    x_ref[...] = x
    enter_layer(x, stretch_mean(x), gain_ref[0:1, :], xn_ref, ms_ref, tail_ref)


def first_step(frames_in, attn_gain):
    return pl.pallas_call(
        first_kernel,
        out_shape=(
            jax.ShapeDtypeStruct((ROWS, D), F32),
            jax.ShapeDtypeStruct((ROWS, D), BF16),
            jax.ShapeDtypeStruct((32, D), BF16),
            jax.ShapeDtypeStruct((PRIOR, D), BF16),
        ),
        in_specs=[HBM, VMEM],
        out_specs=(VMEM, VMEM, VMEM, VMEM),
        scratch_shapes=[pltpu.VMEM((ROWS, D), BF16), pltpu.SemaphoreType.DMA],
        compiler_params=SMALL,
        name="first_step",
    )(frames_in, attn_gain)


def back_product(inputs, weight):
    return lax.dot_general(inputs, weight, (((1,), (1,)), ((), ())), preferred_element_type=F32)


def gelu(values):
    return 0.5 * values * (1.0 + lax.erf(values * (2.0**-0.5)))


def layer_kernel(last, layer, lengths_ref, x_ref, xn_ref, ms_ref, prior_ref, fgain_ref, again_ref, *rest):
    pieces, rest = rest[:10], rest[10:]
    if last:
        out_ref, *scratch = rest
    else:
        x_out, xn_out, ms_out, tail_out, *scratch = rest
    w, kin, qin, ks, vs, qs, os_, bias, sems = scratch
    core, x_at, y_at, _, seq_rank = place()

    def fetch(from_core, arrays):
        groups = ((0, 0, 4), (1, 4, 6)) if from_core == 0 else ((1, 6, 12),)
        for sem, start, stop in groups:
            group, part = slice(start, stop), slice(start - 6 * from_core, stop - 6 * from_core)
            for array, (by, z_start, z_stop) in zip(arrays, PIECES):
                src = array.reshape(z_stop - z_start, 4, 6, 16, 128)
                z_rows = slice(z_start, z_stop)
                if from_core == 0:
                    cols = pl.ds(pl.multiple_of(((y_at + by) & 3) * 128, 128), 128)
                    dst = w.at[z_rows, :, group, :, cols]
                    pltpu.make_async_copy(src.at[:, :, part], dst, sems.at[sem]).start()
                else:
                    for y in range(4):
                        dst = w.at[z_rows, (x_at + by) & 3, group, :, 128 * y : 128 * y + 128]
                        pltpu.make_async_copy(src.at[:, y, part], dst, sems.at[sem]).start()

    @pl.when(core == 0)
    def _():
        fetch(0, pieces[:5])
        fetch(1, pieces[5:])

    @pl.when(core != 0)
    def _():
        fetch(0, pieces[5:])
        fetch(1, pieces[:5])

    def arrived(sem, group):
        pltpu.make_async_copy(w.at[:, :, group], w.at[:, :, group], sems.at[sem]).wait()

    def matrix(j):
        return w[:, :, j].reshape(D, D)

    first_stretch = seq_rank * GROUPS
    kin[0:LEFT, :] = prior_ref[0:LEFT, :]
    kin[LEFT : LEFT + ROWS, :] = xn_ref[...]
    kin[320:336, :] = prior_ref[LEFT:PRIOR, :]
    kin[336:352, :] = ms_ref[0:16, :]
    kin[352:384, :] = jnp.zeros((32, D), BF16)
    qin[0:ROWS, :] = xn_ref[...]
    qin[ROWS:QUERIES, :] = ms_ref[16:32, :]
    row = lax.broadcasted_iota(jnp.int32, (QUERIES, KEYS), 0)
    col = lax.broadcasted_iota(jnp.int32, (QUERIES, KEYS), 1)
    stretch = jnp.where(row < ROWS, row // STRETCH, (row - ROWS) % GROUPS)
    frame_from = col // STRETCH - LEFT // STRETCH
    memory_from = jnp.where(col < 336, col - 320 - MEMORY, col - 336)
    memory_there = col < jnp.where(col < 336, 320 + MEMORY, 336 + GROUPS)
    is_frame = col < LEFT + ROWS
    source = jnp.where(is_frame, frame_from, memory_from)
    back = stretch - source
    seen_frame = is_frame & (back >= 0) & (back <= LEFT // STRETCH)
    seen_memory = (~is_frame) & memory_there & (back >= 1) & (back <= MEMORY)
    allowed = (seen_frame | seen_memory) & (source + first_stretch >= 0)
    bias[...] = jnp.where(allowed, 0.0, MASKED)

    arrived(0, slice(0, 4))
    q = jnp.dot(qin[...], matrix(0), preferred_element_type=F32)
    qs[...] = (q * HEAD_DIM ** (-0.5)).astype(BF16)
    ks[...] = jnp.dot(kin[...], matrix(1), preferred_element_type=F32).astype(BF16)
    vs[...] = jnp.dot(kin[...], matrix(2), preferred_element_type=F32).astype(BF16)
    lane = lax.broadcasted_iota(jnp.int32, (QUERIES, 128), 1)
    for pair in range(D // 128):
        cols = slice(128 * pair, 128 * pair + 128)
        queries, keys, values = qs[:, cols], ks[:, cols], vs[:, cols]
        mixed = []
        for half in range(2):
            mine = (lane < HEAD_DIM) if half == 0 else (lane >= HEAD_DIM)
            scores = back_product(jnp.where(mine, queries, jnp.zeros_like(queries)), keys) + bias[...]
            highest = jnp.max(scores, axis=-1, keepdims=True)
            exponent = jnp.exp(scores - highest)
            total = jnp.sum(exponent, axis=-1, keepdims=True)
            product = jnp.dot(exponent.astype(BF16), values, preferred_element_type=F32)
            mixed.append(product * (1.0 / total))
        os_[:, cols] = jnp.where(lane < HEAD_DIM, mixed[0], mixed[1]).astype(BF16)
    projected = back_product(os_[...], matrix(3))
    x = x_ref[...] + projected[0:ROWS]
    hn = norm(x, fgain_ref[layer : layer + 1, :])
    arrived(1, slice(4, 12))
    for part in range(4):
        hidden = gelu(jnp.dot(hn, matrix(4 + part), preferred_element_type=F32)).astype(BF16)
        x = x + back_product(hidden, matrix(8 + part))
    if last:
        length = lengths_ref[y_at]
        position = STRETCH * first_stretch + lax.broadcasted_iota(jnp.int32, (ROWS, D), 0)
        out_ref[...] = jnp.where(position < length, x, 0.0).astype(BF16)
    else:
        x_out[...] = x
        memory = projected[ROWS : ROWS + GROUPS]
        enter_layer(x, memory, again_ref[layer + 1 : layer + 2, :], xn_out, ms_out, tail_out)


def layer_step(layer, last, lengths, x, xn, ms, prior, ffn_gain, attn_gain, weights):
    def kernel(*refs):
        layer_kernel(last, layer, *refs)

    if last:
        out_shape = jax.ShapeDtypeStruct((ROWS, D), BF16)
        out_specs = VMEM
    else:
        out_shape = (
            jax.ShapeDtypeStruct((ROWS, D), F32),
            jax.ShapeDtypeStruct((ROWS, D), BF16),
            jax.ShapeDtypeStruct((32, D), BF16),
            jax.ShapeDtypeStruct((PRIOR, D), BF16),
        )
        out_specs = (VMEM, VMEM, VMEM, VMEM)
    return pl.pallas_call(
        kernel,
        out_shape=out_shape,
        in_specs=[SMEM, VMEM, VMEM, VMEM, VMEM, VMEM, VMEM] + [HBM] * 10,
        out_specs=out_specs,
        scratch_shapes=[
            pltpu.VMEM((8, 4, 12, 16, D), BF16),
            pltpu.VMEM((KEYS, D), BF16),
            pltpu.VMEM((QUERIES, D), BF16),
            pltpu.VMEM((KEYS, D), BF16),
            pltpu.VMEM((KEYS, D), BF16),
            pltpu.VMEM((QUERIES, D), BF16),
            pltpu.VMEM((QUERIES, D), BF16),
            pltpu.VMEM((QUERIES, KEYS), F32),
            pltpu.SemaphoreType.DMA((2,)),
        ],
        compiler_params=pltpu.CompilerParams(vmem_limit_bytes=32 * 1024 * 1024),
        name="layer_step_%d" % layer,
    )(lengths, x, xn, ms, prior, ffn_gain, attn_gain, *weights)


def from_behind(array):
    devices = lax.axis_size("seq")
    return lax.ppermute(array, "seq", [(i, i + 1) for i in range(devices - 1)])


def weight_blocks(qkv_weight, out_weight, up_weight, down_weight):
    def wide(weight):
        return jnp.moveaxis(weight.reshape(2, 8, 4, 128), 2, 1)

    return jnp.concatenate([qkv_weight, out_weight[:, None], wide(up_weight), wide(down_weight)], axis=1)


def by_chip(move):
    pairs = []
    for x in range(4):
        for core in range(2):
            for y in range(4):
                to_x, to_core, to_y = move(x, core, y)
                pairs.append(((2 * x + core) * 4 + y, (2 * (to_x % 4) + to_core) * 4 + to_y % 4))
    return pairs


def to_partner(array):
    return lax.ppermute(array, ("seq", "mp"), by_chip(lambda x, core, y: (x, 1 - core, y)))


def around(array, along_x_core, by):
    def move(x, core, y):
        return (x + by, core, y) if core == along_x_core else (x, core, y + by)

    return lax.ppermute(array, ("seq", "mp"), by_chip(move))


def along_mp(array, by):
    return lax.ppermute(array, "mp", [(y, (y + by) % 4) for y in range(4)])


def neighbours(array, send):
    return send(array, 1), send(array, -1)


def opposite(from_behind_piece, from_ahead_piece, send):
    half = from_behind_piece.shape[0] // 2
    return send(from_behind_piece[:half], 1), send(from_ahead_piece[half:], -1)


def join_ring_kernel(*refs):
    pieces, outs = refs[:5], refs[-2:]
    core, x_at, y_at, _, _ = place()
    own = jnp.where(core == 0, x_at, y_at)
    for piece, (by, z_start, z_stop) in zip(pieces, PIECES):
        at = (own + by) & 3
        for z in range(z_start, z_stop):
            for layer in range(2):
                rows = slice(12 * (z - z_start) + 6 * layer, 12 * (z - z_start) + 6 * layer + 6)
                outs[layer][pl.ds((4 * z + at) * 6, 6)] = piece[rows]


def join_ring(pieces, after):
    part = jax.ShapeDtypeStruct((192, 16, 128), BF16)
    return pl.pallas_call(
        join_ring_kernel,
        out_shape=(part, part),
        in_specs=[VMEM] * 5 + [HBM],
        out_specs=(VMEM, VMEM),
        compiler_params=SMALL,
        name="join_ring",
    )(*pieces, after)


def join_rows_kernel(*refs):
    pieces, out, sem = refs[:5], refs[5], refs[6]
    _, _, y_at, _, _ = place()
    copies = []
    for at, (piece, (by, start, stop)) in enumerate(zip(pieces, PIECES)):
        dst = out.at[(y_at + by) & 3, ROWS // 8 * start : ROWS // 8 * stop]
        copies.append(pltpu.make_async_copy(piece, dst, sem.at[at]))
    for copy in copies:
        copy.start()
    for copy in copies:
        copy.wait()


def join_rows(pieces):
    return pl.pallas_call(
        join_rows_kernel,
        out_shape=jax.ShapeDtypeStruct((4, ROWS, D), BF16),
        in_specs=[VMEM] * 5,
        out_specs=HBM,
        scratch_shapes=[pltpu.SemaphoreType.DMA((5,))],
        compiler_params=SMALL,
        name="join_rows",
    )(*pieces)


def first_ring(array, by):
    return around(array, 0, by)


def second_ring(array, by):
    return around(array, 1, by)


def first_rings(core, blocks, after):
    mine = lax.dynamic_slice_in_dim(blocks, 6 * core, 6, 1)
    other = to_partner(lax.dynamic_slice_in_dim(blocks, 6 * (1 - core), 6, 1))
    first = jnp.where(core == 0, mine, other)
    second = jnp.where(core == 0, other, mine)
    both = jnp.concatenate([first, second], axis=2).reshape(12, 16, 128)
    copies = jnp.broadcast_to(both, (8, *both.shape))
    over_z = lax.all_to_all(copies, "dp", split_axis=0, concat_axis=0, tiled=True).reshape(96, 16, 128)
    behind, ahead = neighbours(over_z, first_ring)
    return join_ring([over_z, behind, ahead, *opposite(behind, ahead, first_ring)], after)


def shards(frames_in, lengths, attn_gain, ffn_gain, qkv_weight, out_weight, up_weight, down_weight):
    core = lax.axis_index("seq") % 2
    x, xn, ms, tail = first_step(frames_in, attn_gain)
    prior = from_behind(tail)
    blocks = weight_blocks(qkv_weight, out_weight, up_weight, down_weight)
    part0, part1 = first_rings(core, blocks, prior)
    behind0, ahead0 = neighbours(part0, second_ring)
    part1, behind0 = lax.optimization_barrier((part1, behind0))
    pieces0 = [part0, behind0, ahead0, *opposite(behind0, ahead0, second_ring)]
    weights0 = pieces0 + [to_partner(piece) for piece in pieces0]
    behind1, ahead1 = neighbours(part1, second_ring)
    x, xn, ms, tail = layer_step(0, False, lengths, x, xn, ms, prior, ffn_gain, attn_gain, weights0)
    tail, part1, behind1, ahead1 = lax.optimization_barrier((tail, part1, behind1, ahead1))
    prior = from_behind(tail)
    pieces1 = [part1, behind1, ahead1, *opposite(behind1, ahead1, second_ring)]
    weights1 = pieces1 + [to_partner(piece) for piece in pieces1]
    encoded = layer_step(1, True, lengths, x, xn, ms, prior, ffn_gain, attn_gain, weights1)
    behind, ahead = neighbours(encoded, along_mp)
    return join_rows([encoded, behind, ahead, *opposite(behind, ahead, along_mp)])


def solution(mesh):
    in_specs = (
        P("dp", "seq", None),
        P("dp"),
        P(),
        P(),
        P(None, None, ("dp", "seq"), "mp"),
        P(None, ("dp", "seq"), "mp"),
        P(None, ("dp", "seq"), "mp"),
        P(None, ("dp", "seq"), "mp"),
    )
    out_specs = P("dp", "seq", None)
    return jax.shard_map(shards, mesh=mesh, in_specs=in_specs, out_specs=out_specs, check_vma=False)
```
